32 devices in a mesh: row: 4 (over z), col: 4 (over y, x), layer: 2 (over core).
Axes of the slice: x: 2, y: 2, z: 4, core: 2. Of those that a mesh axis runs over, the one named last changes fastest.
Arguments:
- expression: bfloat16 [6144, 1024], P(('row', 'col'), 'layer'), may hold values from -240 to 240
Outputs:
- connectivity: float32 [6144], P(('row', 'col', 'layer'))
The draws below stay inside these ranges and needn't reach their ends.
All inputs are finite; a program needn't handle non-finite values.
Results may differ from the reference program's by a relative error of at most 0.00048.
Values may be sent and summed in bfloat16 or wider, within the bound.
A program may use at most 64 MiB of HBM per device.

```python
import math
import jax
import jax.numpy as jnp
from jax import lax

S = 1024
G = 6144


module_count = 384


membership = 3


def draw_expression(key, part):
    keys = jax.random.split(key, 7)
    modules = jax.random.randint(keys[0], (G, membership), 0, module_count)
    loading = jax.random.uniform(keys[1], (G, membership), jnp.float32, -1.0, 1.0)
    factor = jax.random.truncated_normal(keys[2], -3.0, 3.0, (module_count, S), jnp.float32)
    white = jax.random.truncated_normal(keys[3], -4.0, 4.0, (G, S), jnp.float32)
    mixing = jax.random.truncated_normal(keys[6], -4.0, 4.0, (S, S), jnp.float32) / jnp.sqrt(jnp.float32(S))
    spread = jnp.exp(jax.random.uniform(keys[4], (G,), jnp.float32, jnp.log(0.5), jnp.log(2.0)))
    offset = jax.random.uniform(keys[5], (G,), jnp.float32, -3.0, 3.0)
    exponent = 0.3
    decay = (1.0 + jnp.arange(S).astype(jnp.float32)) ** (-exponent)
    decay = decay / jnp.sqrt(jnp.mean(decay * decay))
    noise = jnp.dot(white * decay[None, :], mixing, precision=lax.Precision.HIGHEST)
    noise = jnp.clip(noise, -5.0, 5.0)
    columns = jnp.arange(module_count)
    load_matrix = jnp.zeros((G, module_count), jnp.float32)
    for member in range(membership):
        picked = (modules[:, member][:, None] == columns[None, :]).astype(jnp.float32)
        load_matrix = load_matrix + picked * loading[:, member][:, None]
    signal = jnp.dot(load_matrix, factor, precision=lax.Precision.HIGHEST)
    weights = 1.0 + 2.0 * jnp.arange(S).astype(jnp.float32) / (S - 1)
    values = offset[:, None] + spread[:, None] * weights[None, :] * (noise + 1.5 * signal)
    return values.astype(jnp.bfloat16)


def setup_inputs(seed: int = 0) -> dict:
    key_of = jax.random.split(jax.random.key(seed), 2)
    return {
        "expression": draw_expression(jax.random.fold_in(key_of[1], 71), 0),
    }


epsilon = 1e-05

def adjacency(correlation):
    shifted = (1.0 + correlation) * 0.5
    square = shifted * shifted
    fourth = square * square
    eighth = fourth * fourth
    return eighth * fourth

def reference(expression):
    values = expression.astype(jnp.float32)
    total = lax.optimization_barrier(jnp.sum(values, axis=1))
    squares = lax.optimization_barrier(jnp.sum(values * values, axis=1))
    average = total / S
    variance = squares / S - average * average
    scaled = ((values - average[:, None]) * lax.rsqrt(variance + epsilon)[:, None]).astype(jnp.bfloat16)
    block_rows = math.gcd(G, 1024)
    grouped = scaled.reshape(G // block_rows, block_rows, S)

    def one_block(segment):
        tile_sum = lax.dot_general(segment, scaled, (((1,), (1,)), ((), ())), preferred_element_type=jnp.float32)
        return lax.optimization_barrier(jnp.sum(adjacency(tile_sum / S), axis=1))
    totals = lax.map(one_block, grouped).reshape(G)
    return totals - 1.0
```

```python
import functools

import jax
import jax.numpy as jnp
from jax import lax
from jax.experimental import pallas as pl
from jax.experimental.pallas import tpu as pltpu
from jax.sharding import PartitionSpec as P

MESH = pl.DeviceIdType.MESH
epsilon = 1e-05


def flip(c, k):
    bit = 1
    while bit <= k:
        if k & bit:
            c = c + bit - 2 * bit * lax.rem(lax.div(c, bit), 2)
        bit *= 2
    return c


def kernel(rows, cols, x_ref, out_ref, peer, own, panel, far, pacc, racc, psrc, pdst, rsrc, rdst,
           ex_sem, ps_sem, pr_sem, zs_sem, zr_sem, xs_sem, xr_sem, qs_sem, qr_sem, ts_sem, tr_sem):
    p, c, l = lax.axis_index("row"), lax.axis_index("col"), lax.axis_index("layer")
    genes, part = x_ref.shape
    half = genes // 2
    samples = 2 * part
    depth = rows // 2
    other = 1 - l

    def remote(src, dst, send, recv, device):
        return pltpu.make_async_remote_copy(
            src_ref=src, dst_ref=dst, send_sem=send, recv_sem=recv, device_id=device, device_id_type=MESH
        )

    barrier = pltpu.get_barrier_semaphore()
    greeted = [(p, c, other)] + [(p, flip(c, k), l) for k in range(1, cols)]
    greeted += [(lax.rem(p + r, rows), c, h) for r in range(1, rows) for h in range(2)]
    for device in greeted:
        pl.semaphore_signal(barrier, inc=1, device_id=device, device_id_type=MESH)
    pl.semaphore_wait(barrier, len(greeted))

    exchange = remote(x_ref, peer, ex_sem.at[0], ex_sem.at[1], (p, c, other))
    exchange.start()
    exchange.wait_recv()

    first = l == 0
    step = 32

    def standardize(h):
        @pl.loop(0, half // step)
        def _(i):
            at = pl.ds(pl.multiple_of(h * half + i * step, step), step)
            mine = x_ref[at, :].astype(jnp.float32)
            theirs = peer[at, :].astype(jnp.float32)
            low = jnp.where(first, mine, theirs)
            high = jnp.where(first, theirs, mine)
            total = jnp.sum(low, axis=1, keepdims=True) + jnp.sum(high, axis=1, keepdims=True)
            squares = jnp.sum(low * low + high * high, axis=1, keepdims=True)
            average = total / samples
            variance = squares / samples - average * average
            gain = lax.rsqrt(variance + epsilon)
            own[at, 0:part] = ((low - average) * gain).astype(jnp.bfloat16)
            own[at, part:samples] = ((high - average) * gain).astype(jnp.bfloat16)

    standardize(l)
    mine_at = pl.ds(pl.multiple_of(l * half, half), half)
    theirs_at = pl.ds(pl.multiple_of(other * half, half), half)

    low_index = lax.rem(p, depth)
    odd = lax.rem(low_index, 2) == 1
    is_low = p < depth
    sends_last = odd == is_low
    receives_last = odd != is_low

    panel_copies = [
        remote(own.at[mine_at], panel.at[c], ps_sem.at[k - 1], pr_sem.at[k - 1], (p, flip(c, k), l))
        for k in range(1, cols)
    ]
    far_copies = [
        remote(own.at[mine_at], far.at[d - 1, mine_at], zs_sem.at[d - 1], zr_sem.at[d - 1],
               (lax.rem(p + d, rows), c, l))
        for d in range(1, depth + 1)
    ]
    for copy in far_copies[:-1]:
        copy.start()
    for copy in panel_copies[:2]:
        copy.start()

    @pl.when(sends_last)
    def _():
        far_copies[-1].start()

    for copy in panel_copies[2:]:
        copy.start()

    standardize(other)
    panel[c] = own[mine_at, :]
    pacc[...] = jnp.zeros_like(pacc)
    racc[...] = jnp.zeros_like(racc)

    def pairs(slot, block, back=None):
        product = lax.dot_general(
            panel[slot], block, (((1,), (1,)), ((), ())), preferred_element_type=jnp.float32
        )
        shifted = product * (0.5 / samples) + 0.5
        square = shifted * shifted
        fourth = square * square
        eighth = fourth * fourth
        value = eighth * fourth
        lanes = value[:, 0:128]
        for j in range(1, genes // 128):
            lanes = lanes + value[:, j * 128:(j + 1) * 128]
        pacc[slot] += lanes
        if back is not None:
            racc[back] += jnp.sum(value.reshape(half // 8, 8, genes), axis=0)

    relays = [
        remote(far.at[d, mine_at], far.at[d, mine_at], xs_sem.at[d], xr_sem.at[d], (p, c, other))
        for d in range(depth)
    ]

    def give_back(d):
        total = racc[d]
        home = lax.rem(p + rows - d - 1, rows)
        for h in range(2):
            rsrc[d, h] = total[:, h * half:(h + 1) * half]
            remote(rsrc.at[d, h], rdst.at[d, l], ts_sem.at[d, h], tr_sem.at[d, l], (home, c, h)).start()

    pairs(c, own[...])
    for k in range(1, cols - 1):
        panel_copies[k - 1].wait_recv()
        pairs(flip(c, k), own[...])
    late = flip(c, cols - 1)
    for d in range(depth - 1):
        far_copies[d].wait_recv()
        relays[d].start()
        relays[d].wait_recv()

        @pl.loop(0, cols - 1)
        def _(j):
            pairs(lax.rem(late + 1 + j, cols), far[d], d)

    @pl.when(receives_last)
    def _():
        far_copies[-1].wait_recv()
        relays[-1].start()

    panel_copies[-1].wait_recv()
    pairs(late, own[...])
    for d in range(depth - 1):
        pairs(late, far[d], d)
        give_back(d)

    @pl.when(receives_last)
    def _():
        relays[-1].wait_recv()

        @pl.loop(0, cols)
        def _(slot):
            pairs(slot, far[depth - 1], depth - 1)

        give_back(depth - 1)

    def fold(slot):
        turned = pacc[slot].T
        return jnp.sum(turned.reshape(128 // 8, 8, half), axis=0)

    part_copies = []
    for k in range(1, cols):
        slot = flip(c, k)
        psrc[k - 1] = fold(slot)
        copy = remote(psrc.at[k - 1], pdst.at[k - 1], qs_sem.at[k - 1], qr_sem.at[k - 1], (p, slot, l))
        copy.start()
        part_copies.append(copy)
    total = fold(c)
    for copy in part_copies:
        copy.wait_recv()
    for k in range(1, cols):
        total = total + pdst[k - 1]

    def back_copy(d, h):
        return remote(rsrc.at[d, h], rdst.at[d, h], ts_sem.at[d, h], tr_sem.at[d, h], (p, c, other))

    for d in range(depth - 1):
        for h in range(2):
            back_copy(d, h).wait_recv()
            total = total + rdst[d, h]
    out_ref[...] = jnp.sum(total, axis=0, keepdims=True) - 1.0

    @pl.when(sends_last)
    def _():
        extra = jnp.zeros_like(total)
        for h in range(2):
            back_copy(depth - 1, h).wait_recv()
            extra = extra + rdst[depth - 1, h]
        out_ref[...] += jnp.sum(extra, axis=0, keepdims=True)
        far_copies[-1].wait_send()

    exchange.wait_send()
    for copy in panel_copies + far_copies[:-1] + relays[:-1] + part_copies:
        copy.wait_send()
    for d in range(depth - 1):
        for h in range(2):
            back_copy(d, h).wait_send()

    @pl.when(receives_last)
    def _():
        relays[-1].wait_send()
        for h in range(2):
            back_copy(depth - 1, h).wait_send()


def solution(mesh):
    rows, cols = mesh.shape["row"], mesh.shape["col"]
    depth = rows // 2
    dma = lambda *shape: pltpu.SemaphoreType.DMA(shape)

    def on_device(expression):
        genes, part = expression.shape
        half, samples = genes // 2, 2 * part
        summed = pl.pallas_call(
            functools.partial(kernel, rows, cols),
            out_shape=jax.ShapeDtypeStruct((1, half), jnp.float32),
            in_specs=[pl.BlockSpec(memory_space=pltpu.VMEM)],
            out_specs=pl.BlockSpec(memory_space=pltpu.VMEM),
            scratch_shapes=[
                pltpu.VMEM((genes, part), jnp.bfloat16),
                pltpu.VMEM((genes, samples), jnp.bfloat16),
                pltpu.VMEM((cols, half, samples), jnp.bfloat16),
                pltpu.VMEM((depth, genes, samples), jnp.bfloat16),
                pltpu.VMEM((cols, half, 128), jnp.float32),
                pltpu.VMEM((depth, 8, genes), jnp.float32),
                pltpu.VMEM((cols - 1, 8, half), jnp.float32),
                pltpu.VMEM((cols - 1, 8, half), jnp.float32),
                pltpu.VMEM((depth, 2, 8, half), jnp.float32),
                pltpu.VMEM((depth, 2, 8, half), jnp.float32),
                dma(2),
                dma(cols - 1), dma(cols - 1),
                dma(depth), dma(depth),
                dma(depth), dma(depth),
                dma(cols - 1), dma(cols - 1),
                dma(depth, 2), dma(depth, 2),
            ],
            compiler_params=pltpu.CompilerParams(collective_id=0, has_side_effects=True),
        )(expression)
        return summed.reshape(half)

    return jax.shard_map(
        on_device,
        mesh=mesh,
        in_specs=(P(("row", "col"), "layer"),),
        out_specs=P(("row", "col", "layer")),
        check_vma=False,
    )
```

```python
import functools

import jax
import jax.numpy as jnp
from jax import lax
from jax.experimental import pallas as pl
from jax.experimental.pallas import tpu as pltpu
from jax.sharding import PartitionSpec as P

MESH = pl.DeviceIdType.MESH
epsilon = 1e-05


def flip(c, k):
    bit = 1
    while bit <= k:
        if k & bit:
            c = c + bit - 2 * bit * lax.rem(lax.div(c, bit), 2)
        bit *= 2
    return c


def kernel(rows, cols, x_ref, out_ref, raw, own, panel, far_raw, far, pacc, racc, psrc, pdst, rsrc, rdst,
           in_sem, ex_sem, ps_sem, pr_sem, zs_sem, zr_sem, xs_sem, xr_sem, qs_sem, qr_sem, ts_sem, tr_sem):
    p, c, l = lax.axis_index("row"), lax.axis_index("col"), lax.axis_index("layer")
    genes, part = x_ref.shape
    half = genes // 2
    samples = 2 * part
    depth, pieces, piece = far.shape[0], far.shape[1], far.shape[2]
    other = 1 - l
    late = flip(c, 3)

    def remote(src, dst, send, recv, device):
        return pltpu.make_async_remote_copy(
            src_ref=src, dst_ref=dst, send_sem=send, recv_sem=recv, device_id=device, device_id_type=MESH
        )

    load = pltpu.make_async_copy(x_ref, raw.at[l], in_sem)
    load.start()

    barrier = pltpu.get_barrier_semaphore()
    greeted = [(lax.rem(p + r, rows), c, h) for r in range(1, rows) for h in range(2)]
    greeted += [(p, flip(c, k), l) for k in range(1, cols)] + [(p, c, other)]
    for device in greeted:
        pl.semaphore_signal(barrier, inc=1, device_id=device, device_id_type=MESH)
    pacc[...] = jnp.zeros_like(pacc)
    racc[...] = jnp.zeros_like(racc)
    load.wait()
    pl.semaphore_wait(barrier, len(greeted))

    odd = lax.rem(lax.rem(p, depth), 2) == 1
    is_low = p < depth
    sends_last = odd == is_low
    receives_last = odd != is_low

    def far_copy(d, i):
        at = pl.ds(pl.multiple_of(i * piece, piece), piece)
        return remote(raw.at[l, at], far_raw.at[d, i, l], zs_sem.at[d, i], zr_sem.at[d, i],
                      (lax.rem(p + d + 1, rows), c, l))

    def relay(d, i):
        return remote(far_raw.at[d, i, l], far_raw.at[d, i, l], xs_sem.at[d, i], xr_sem.at[d, i], (p, c, other))

    for d in range(depth - 1):
        for i in range(pieces):
            far_copy(d, i).start()

    @pl.when(sends_last)
    def _():
        for i in range(pieces):
            far_copy(depth - 1, i).start()

    exchange = remote(raw.at[l], raw.at[l], ex_sem.at[0], ex_sem.at[1], (p, c, other))
    exchange.start()
    exchange.wait_recv()

    step = 32

    def scale(low, high):
        low, high = low.astype(jnp.float32), high.astype(jnp.float32)
        total = jnp.sum(low, axis=1, keepdims=True) + jnp.sum(high, axis=1, keepdims=True)
        squares = jnp.sum(low * low + high * high, axis=1, keepdims=True)
        average = total / samples
        variance = squares / samples - average * average
        gain = lax.rsqrt(variance + epsilon)
        return (((low - average) * gain).astype(jnp.bfloat16), ((high - average) * gain).astype(jnp.bfloat16))

    def standardize(h):
        @pl.loop(0, half // step)
        def _(i):
            at = pl.ds(pl.multiple_of(h * half + i * step, step), step)
            low, high = scale(raw[0, at, :], raw[1, at, :])
            own[at, 0:part] = low
            own[at, part:samples] = high

    def standardize_far(d, i):
        @pl.loop(0, piece // step)
        def _(j):
            at = pl.ds(pl.multiple_of(j * step, step), step)
            low, high = scale(far_raw[d, i, 0, at, :], far_raw[d, i, 1, at, :])
            far[d, i, at, 0:part] = low
            far[d, i, at, part:samples] = high

    standardize(l)
    mine_at = pl.ds(pl.multiple_of(l * half, half), half)
    cut = half // 2

    def panel_copy(k, s):
        at = pl.ds(pl.multiple_of(l * half + s * cut, cut), cut)
        return remote(own.at[at], panel.at[c, pl.ds(s * cut, cut)], ps_sem.at[k - 1, s], pr_sem.at[k - 1, s],
                      (p, flip(c, k), l))

    def pass_on(s):
        slot, target = (flip(c, 2), flip(c, 1)) if s == 0 else (flip(c, 1), flip(c, 2))
        at = pl.ds(s * cut, cut)
        return remote(panel.at[slot, at], panel.at[slot, at], ps_sem.at[2, s], pr_sem.at[2, s], (p, target, l))

    direct = [k for k in range(1, cols) if k != 3]
    panel_copies = {(k, s): panel_copy(k, s) for k in direct for s in range(2)}
    panel_copies.update({(3, s): pass_on(s) for s in range(2)})
    for k, s in [(1, 1), (2, 0), (1, 0), (2, 1)] + [(k, s) for k in direct[2:] for s in range(2)]:
        panel_copies[k, s].start()

    standardize(other)
    panel[c] = own[mine_at, :]

    def adjacency(slot, block):
        product = lax.dot_general(
            panel[slot], block, (((1,), (1,)), ((), ())), preferred_element_type=jnp.float32
        )
        shifted = product * (0.5 / samples) + 0.5
        square = shifted * shifted
        fourth = square * square
        eighth = fourth * fourth
        return eighth * fourth

    def own_pairs(slot):
        value = adjacency(slot, own[...])
        lanes = value[:, 0:128]
        for j in range(1, genes // 128):
            lanes = lanes + value[:, j * 128:(j + 1) * 128]
        pacc[slot] += lanes

    def far_pairs(slot, d, i):
        value = adjacency(slot, far[d, i])
        pacc[slot] += value
        racc[d, i] += jnp.sum(value.reshape(half // 8, 8, piece), axis=0)

    count = pieces * jnp.where(receives_last, depth, depth - 1)
    blocks = jnp.where(receives_last, depth, depth - 1)
    mixed = p == 0

    def event(e):
        d = jnp.where(mixed, lax.rem(e, blocks), lax.div(e, pieces))
        i = jnp.where(mixed, lax.div(e, blocks), lax.rem(e, pieces))
        return d, i

    own_pairs(c)
    for s in range(2):
        panel_copies[2 - s, s].wait_recv()
        panel_copies[3, s].start()

    def take(e):
        d, i = event(e)
        far_copy(d, i).wait_recv()
        relay(d, i).start()

    def ready(e):
        d, i = event(e)
        relay(d, i).wait_recv()
        standardize_far(d, i)

    take(0)
    ready(0)
    for s in range(2):
        panel_copies[1 + s, s].wait_recv()
    for k in direct[2:]:
        for s in range(2):
            panel_copies[k, s].wait_recv()
    for k in direct:
        own_pairs(flip(c, k))

    @pl.loop(0, count - 2)
    def _(e):
        @pl.when(e > 0)
        def _():
            take(e)
            ready(e)

        d, i = event(e)

        @pl.loop(0, cols - 1)
        def _(j):
            far_pairs(lax.rem(late + 1 + j, cols), d, i)

    for s in range(2):
        panel_copies[3, s].wait_recv()
    own_pairs(late)

    @pl.loop(0, count - 2)
    def _(e):
        d, i = event(e)
        far_pairs(late, d, i)

    take(count - 2)
    take(count - 1)

    @pl.loop(count - 2, count)
    def _(e):
        ready(e)
        d, i = event(e)

        @pl.loop(0, cols)
        def _(slot):
            far_pairs(slot, d, i)

    def fold(slot):
        turned = pacc[slot].T
        return jnp.sum(turned.reshape(128 // 8, 8, half), axis=0)

    def give_back(d):
        total = jnp.concatenate([racc[d, i] for i in range(pieces)], axis=1)
        home = lax.rem(p + rows - d - 1, rows)
        for h in range(2):
            rsrc[d, h] = total[:, h * half:(h + 1) * half]
            remote(rsrc.at[d, h], rdst.at[d, l], ts_sem.at[d, h], tr_sem.at[d, l], (home, c, h)).start()

    for d in range(depth - 1):
        give_back(d)

    @pl.when(receives_last)
    def _():
        give_back(depth - 1)

    part_copies = []
    for k in range(cols - 1, 0, -1):
        slot = flip(c, k)
        psrc[k - 1] = fold(slot)
        copy = remote(psrc.at[k - 1], pdst.at[k - 1], qs_sem.at[k - 1], qr_sem.at[k - 1], (p, slot, l))
        copy.start()
        part_copies.append(copy)
    total = fold(c)
    for copy in part_copies:
        copy.wait_recv()
    for k in range(1, cols):
        total = total + pdst[k - 1]

    def back_copy(d, h):
        return remote(rsrc.at[d, h], rdst.at[d, h], ts_sem.at[d, h], tr_sem.at[d, h], (p, c, other))

    for d in range(depth - 1):
        for h in range(2):
            back_copy(d, h).wait_recv()
            total = total + rdst[d, h]
    out_ref[...] = total

    @pl.when(sends_last)
    def _():
        extra = jnp.zeros_like(total)
        for h in range(2):
            back_copy(depth - 1, h).wait_recv()
            extra = extra + rdst[depth - 1, h]
        out_ref[...] += extra
        for i in range(pieces):
            far_copy(depth - 1, i).wait_send()

    exchange.wait_send()
    for copy in list(panel_copies.values()) + part_copies:
        copy.wait_send()
    for d in range(depth - 1):
        for i in range(pieces):
            far_copy(d, i).wait_send()
            relay(d, i).wait_send()
        for h in range(2):
            back_copy(d, h).wait_send()

    @pl.when(receives_last)
    def _():
        for i in range(pieces):
            relay(depth - 1, i).wait_send()
        for h in range(2):
            back_copy(depth - 1, h).wait_send()


def solution(mesh):
    rows, cols = mesh.shape["row"], mesh.shape["col"]
    depth = rows // 2
    piece = 128
    dma = lambda *shape: pltpu.SemaphoreType.DMA(shape)

    def on_device(expression):
        genes, part = expression.shape
        half, samples, pieces = genes // 2, 2 * part, genes // piece
        summed = pl.pallas_call(
            functools.partial(kernel, rows, cols),
            out_shape=jax.ShapeDtypeStruct((8, half), jnp.float32),
            in_specs=[pl.BlockSpec(memory_space=pl.ANY)],
            out_specs=pl.BlockSpec(memory_space=pltpu.VMEM),
            scratch_shapes=[
                pltpu.VMEM((2, genes, part), jnp.bfloat16),
                pltpu.VMEM((genes, samples), jnp.bfloat16),
                pltpu.VMEM((cols, half, samples), jnp.bfloat16),
                pltpu.VMEM((depth, pieces, 2, piece, part), jnp.bfloat16),
                pltpu.VMEM((depth, pieces, piece, samples), jnp.bfloat16),
                pltpu.VMEM((cols, half, 128), jnp.float32),
                pltpu.VMEM((depth, pieces, 8, piece), jnp.float32),
                pltpu.VMEM((cols - 1, 8, half), jnp.float32),
                pltpu.VMEM((cols - 1, 8, half), jnp.float32),
                pltpu.VMEM((depth, 2, 8, half), jnp.float32),
                pltpu.VMEM((depth, 2, 8, half), jnp.float32),
                pltpu.SemaphoreType.DMA,
                dma(2),
                dma(cols - 1, 2), dma(cols - 1, 2),
                dma(depth, pieces), dma(depth, pieces),
                dma(depth, pieces), dma(depth, pieces),
                dma(cols - 1), dma(cols - 1),
                dma(depth, 2), dma(depth, 2),
            ],
            compiler_params=pltpu.CompilerParams(collective_id=0, has_side_effects=True),
        )(expression)
        return jnp.sum(summed, axis=0) - 1.0

    return jax.shard_map(
        on_device,
        mesh=mesh,
        in_specs=(P(("row", "col"), "layer"),),
        out_specs=P(("row", "col", "layer")),
        check_vma=False,
    )
```

```python
import functools

import jax
import jax.numpy as jnp
from jax import lax
from jax.experimental import pallas as pl
from jax.experimental.pallas import tpu as pltpu
from jax.sharding import PartitionSpec as P

MESH = pl.DeviceIdType.MESH
epsilon = 1e-05


def flip(c, k):
    bit = 1
    while bit <= k:
        if k & bit:
            c = c + bit - 2 * bit * lax.rem(lax.div(c, bit), 2)
        bit *= 2
    return c


def kernel(rows, cols, x_ref, out_ref, raw, own, panel, far_raw, far, pacc, racc, psrc, pdst, rsrc, rdst,
           in_sem, ex_sem, ps_sem, pr_sem, zs_sem, zr_sem, xs_sem, xr_sem, qs_sem, qr_sem, ts_sem, tr_sem):
    p, c, l = lax.axis_index("row"), lax.axis_index("col"), lax.axis_index("layer")
    genes, part = x_ref.shape
    half = genes // 2
    samples = 2 * part
    depth, pieces, piece = far.shape[0], far.shape[1], far.shape[2]
    other = 1 - l
    order = [k for k in range(cols) if k != 3] + [3]
    last = cols - 1

    def rows_of(first, stop):
        return pl.ds(first * half, (stop - first) * half)

    def remote(src, dst, send, recv, device):
        return pltpu.make_async_remote_copy(
            src_ref=src, dst_ref=dst, send_sem=send, recv_sem=recv, device_id=device, device_id_type=MESH
        )

    load = pltpu.make_async_copy(x_ref, raw.at[l], in_sem)
    load.start()

    barrier = pltpu.get_barrier_semaphore()
    greeted = [(lax.rem(p + r, rows), c, h) for r in range(1, rows) for h in range(2)]
    greeted += [(p, flip(c, k), l) for k in range(1, cols)] + [(p, c, other)]
    for device in greeted:
        pl.semaphore_signal(barrier, inc=1, device_id=device, device_id_type=MESH)
    pacc[...] = jnp.zeros_like(pacc)
    racc[...] = jnp.zeros_like(racc)
    load.wait()
    pl.semaphore_wait(barrier, len(greeted))

    odd = lax.rem(lax.rem(p, depth), 2) == 1
    is_low = p < depth
    sends_last = odd == is_low
    receives_last = odd != is_low

    def far_copy(d, i):
        at = pl.ds(pl.multiple_of(i * piece, piece), piece)
        return remote(raw.at[l, at], far_raw.at[d, i, l], zs_sem.at[d, i], zr_sem.at[d, i],
                      (lax.rem(p + d + 1, rows), c, l))

    def relay(d, i):
        return remote(far_raw.at[d, i, l], far_raw.at[d, i, l], xs_sem.at[d, i], xr_sem.at[d, i], (p, c, other))

    for d in range(depth - 1):
        for i in range(pieces):
            far_copy(d, i).start()

    @pl.when(sends_last)
    def _():
        for i in range(pieces):
            far_copy(depth - 1, i).start()

    exchange = remote(raw.at[l], raw.at[l], ex_sem.at[0], ex_sem.at[1], (p, c, other))
    exchange.start()
    exchange.wait_recv()

    step = 32

    def scale(low, high):
        low, high = low.astype(jnp.float32), high.astype(jnp.float32)
        total = jnp.sum(low, axis=1, keepdims=True) + jnp.sum(high, axis=1, keepdims=True)
        squares = jnp.sum(low * low + high * high, axis=1, keepdims=True)
        average = total / samples
        variance = squares / samples - average * average
        gain = lax.rsqrt(variance + epsilon)
        return (((low - average) * gain).astype(jnp.bfloat16), ((high - average) * gain).astype(jnp.bfloat16))

    def standardize(h):
        @pl.loop(0, half // step)
        def _(i):
            at = pl.ds(pl.multiple_of(h * half + i * step, step), step)
            low, high = scale(raw[0, at, :], raw[1, at, :])
            own[at, 0:part] = low
            own[at, part:samples] = high

    def standardize_far(d, i):
        @pl.loop(0, piece // step)
        def _(j):
            at = pl.ds(pl.multiple_of(j * step, step), step)
            low, high = scale(far_raw[d, i, 0, at, :], far_raw[d, i, 1, at, :])
            far[d, i, at, 0:part] = low
            far[d, i, at, part:samples] = high

    standardize(l)
    mine_at = pl.ds(pl.multiple_of(l * half, half), half)
    cut = half // 2

    def panel_copy(k, s):
        at = pl.ds(pl.multiple_of(l * half + s * cut, cut), cut)
        return remote(own.at[at], panel.at[pl.ds(order.index(k) * half + s * cut, cut)], ps_sem.at[k - 1, s], pr_sem.at[k - 1, s],
                      (p, flip(c, k), l))

    def pass_on(s):
        source, target = (2, 1) if s == 0 else (1, 2)
        return remote(panel.at[pl.ds(source * half + s * cut, cut)], panel.at[pl.ds(last * half + s * cut, cut)],
                      ps_sem.at[2, s], pr_sem.at[2, s], (p, flip(c, target), l))

    direct = [k for k in range(1, cols) if k != 3]
    panel_copies = {(k, s): panel_copy(k, s) for k in direct for s in range(2)}
    panel_copies.update({(3, s): pass_on(s) for s in range(2)})
    for k, s in [(1, 1), (2, 0), (1, 0), (2, 1)] + [(k, s) for k in direct[2:] for s in range(2)]:
        panel_copies[k, s].start()

    standardize(other)
    panel[rows_of(0, 1), :] = own[mine_at, :]

    def adjacency(at, block):
        product = lax.dot_general(
            panel[at, :], block, (((1,), (1,)), ((), ())), preferred_element_type=jnp.float32
        )
        shifted = product * (0.5 / samples) + 0.5
        square = shifted * shifted
        fourth = square * square
        eighth = fourth * fourth
        return eighth * fourth

    def own_pairs(first, stop):
        at = rows_of(first, stop)
        value = adjacency(at, own[...])
        lanes = value[:, 0:128]
        for j in range(1, genes // 128):
            lanes = lanes + value[:, j * 128:(j + 1) * 128]
        pacc[at, :] += lanes

    def far_pairs(first, stop, e):
        d, i = event(e)
        at = rows_of(first, stop)
        value = adjacency(at, far[d, i])
        pacc[at, :] += value
        racc[d, i] += jnp.sum(value.reshape(value.shape[0] // 8, 8, piece), axis=0)

    count = pieces * jnp.where(receives_last, depth, depth - 1)
    blocks = jnp.where(receives_last, depth, depth - 1)
    mixed = p == 0

    def event(e):
        d = jnp.where(mixed, lax.rem(e, blocks), lax.div(e, pieces))
        i = jnp.where(mixed, lax.div(e, blocks), lax.rem(e, pieces))
        return d, i

    own_pairs(0, 1)
    for s in range(2):
        panel_copies[2 - s, s].wait_recv()
        panel_copies[3, s].start()

    def take(e):
        d, i = event(e)
        far_copy(d, i).wait_recv()
        relay(d, i).start()

    def ready(e):
        d, i = event(e)
        relay(d, i).wait_recv()
        standardize_far(d, i)

    take(0)
    take(1)
    ready(0)
    take(2)
    ready(1)
    for s in range(2):
        panel_copies[1 + s, s].wait_recv()
    for k in direct[2:]:
        for s in range(2):
            panel_copies[k, s].wait_recv()
    own_pairs(1, last)
    longer = count > 3

    @pl.when(longer)
    def _():
        take(3)

    @pl.loop(0, count - 2)
    def _(e):
        @pl.when(e > 1)
        def _():
            @pl.when(e > 3)
            def _():
                take(e)

            ready(e)

        far_pairs(0, last, e)

    for s in range(2):
        panel_copies[3, s].wait_recv()
    own_pairs(last, cols)

    @pl.loop(0, count - 2)
    def _(e):
        far_pairs(last, cols, e)

    @pl.when(longer)
    def _():
        take(count - 2)
        take(count - 1)
        ready(count - 2)

    far_pairs(0, cols, count - 2)
    ready(count - 1)
    far_pairs(0, cols, count - 1)

    def fold(k):
        at = order.index(k)
        turned = pacc[rows_of(at, at + 1), :].T
        return jnp.sum(turned.reshape(128 // 8, 8, half), axis=0)

    def give_back(d):
        total = jnp.concatenate([racc[d, i] for i in range(pieces)], axis=1)
        home = lax.rem(p + rows - d - 1, rows)
        for h in range(2):
            rsrc[d, h] = total[:, h * half:(h + 1) * half]
            remote(rsrc.at[d, h], rdst.at[d, l], ts_sem.at[d, h], tr_sem.at[d, l], (home, c, h)).start()

    for d in range(depth - 1):
        give_back(d)

    @pl.when(receives_last)
    def _():
        give_back(depth - 1)

    part_copies = []
    for k in range(cols - 1, 0, -1):
        psrc[k - 1] = fold(k)
        copy = remote(psrc.at[k - 1], pdst.at[k - 1], qs_sem.at[k - 1], qr_sem.at[k - 1], (p, flip(c, k), l))
        copy.start()
        part_copies.append(copy)
    total = fold(0) - 1.0 / 8
    for copy in part_copies:
        copy.wait_recv()
    for k in range(1, cols):
        total = total + pdst[k - 1]

    def back_copy(d, h):
        return remote(rsrc.at[d, h], rdst.at[d, h], ts_sem.at[d, h], tr_sem.at[d, h], (p, c, other))

    for d in range(depth - 1):
        for h in range(2):
            back_copy(d, h).wait_recv()
            total = total + rdst[d, h]
    out_ref[...] = total

    @pl.when(sends_last)
    def _():
        extra = jnp.zeros_like(total)
        for h in range(2):
            back_copy(depth - 1, h).wait_recv()
            extra = extra + rdst[depth - 1, h]
        out_ref[...] += extra
        for i in range(pieces):
            far_copy(depth - 1, i).wait_send()

    exchange.wait_send()
    for copy in list(panel_copies.values()) + part_copies:
        copy.wait_send()
    for d in range(depth - 1):
        for i in range(pieces):
            far_copy(d, i).wait_send()
            relay(d, i).wait_send()
        for h in range(2):
            back_copy(d, h).wait_send()

    @pl.when(receives_last)
    def _():
        for i in range(pieces):
            relay(depth - 1, i).wait_send()
        for h in range(2):
            back_copy(depth - 1, h).wait_send()


def solution(mesh):
    rows, cols = mesh.shape["row"], mesh.shape["col"]
    depth = rows // 2
    piece = 128
    dma = lambda *shape: pltpu.SemaphoreType.DMA(shape)

    def on_device(expression):
        genes, part = expression.shape
        half, samples, pieces = genes // 2, 2 * part, genes // piece
        summed = pl.pallas_call(
            functools.partial(kernel, rows, cols),
            out_shape=jax.ShapeDtypeStruct((8, half), jnp.float32),
            in_specs=[pl.BlockSpec(memory_space=pl.ANY)],
            out_specs=pl.BlockSpec(memory_space=pltpu.VMEM),
            scratch_shapes=[
                pltpu.VMEM((2, genes, part), jnp.bfloat16),
                pltpu.VMEM((genes, samples), jnp.bfloat16),
                pltpu.VMEM((cols * half, samples), jnp.bfloat16),
                pltpu.VMEM((depth, pieces, 2, piece, part), jnp.bfloat16),
                pltpu.VMEM((depth, pieces, piece, samples), jnp.bfloat16),
                pltpu.VMEM((cols * half, 128), jnp.float32),
                pltpu.VMEM((depth, pieces, 8, piece), jnp.float32),
                pltpu.VMEM((cols - 1, 8, half), jnp.float32),
                pltpu.VMEM((cols - 1, 8, half), jnp.float32),
                pltpu.VMEM((depth, 2, 8, half), jnp.float32),
                pltpu.VMEM((depth, 2, 8, half), jnp.float32),
                pltpu.SemaphoreType.DMA,
                dma(2),
                dma(cols - 1, 2), dma(cols - 1, 2),
                dma(depth, pieces), dma(depth, pieces),
                dma(depth, pieces), dma(depth, pieces),
                dma(cols - 1), dma(cols - 1),
                dma(depth, 2), dma(depth, 2),
            ],
            compiler_params=pltpu.CompilerParams(collective_id=0, has_side_effects=True),
        )(expression)
        return jnp.sum(summed, axis=0)

    return jax.shard_map(
        on_device,
        mesh=mesh,
        in_specs=(P(("row", "col"), "layer"),),
        out_specs=P(("row", "col", "layer")),
        check_vma=False,
    )
```

```python
import functools

import jax
import jax.numpy as jnp
from jax import lax
from jax.experimental import pallas as pl
from jax.experimental.pallas import tpu as pltpu
from jax.sharding import PartitionSpec as P

MESH = pl.DeviceIdType.MESH
epsilon = 1e-05


def flip(c, k):
    bit = 1
    while bit <= k:
        if k & bit:
            c = c + bit - 2 * bit * lax.rem(lax.div(c, bit), 2)
        bit *= 2
    return c


def kernel(rows, cols, x_ref, out_ref, raw, own, panel, far_raw, far, pacc, racc, psrc, pdst, rsrc, rdst,
           in_sem, ex_sem, ps_sem, pr_sem, zs_sem, zr_sem, xs_sem, xr_sem, qs_sem, qr_sem, ts_sem, tr_sem):
    p, c, l = lax.axis_index("row"), lax.axis_index("col"), lax.axis_index("layer")
    genes, part = x_ref.shape
    half = genes // 2
    samples = 2 * part
    depth, pieces, piece = far.shape[0], far.shape[1], far.shape[2]
    other = 1 - l
    order = [k for k in range(cols) if k != 3] + [3]
    last = cols - 1

    def rows_of(first, stop):
        return pl.ds(first * half, (stop - first) * half)

    def remote(src, dst, send, recv, device):
        return pltpu.make_async_remote_copy(
            src_ref=src, dst_ref=dst, send_sem=send, recv_sem=recv, device_id=device, device_id_type=MESH
        )

    load = pltpu.make_async_copy(x_ref, raw.at[l], in_sem)
    load.start()

    barrier = pltpu.get_barrier_semaphore()
    greeted = [(lax.rem(p + r, rows), c, h) for r in range(1, rows) for h in range(2)]
    greeted += [(p, flip(c, k), l) for k in range(1, cols)] + [(p, c, other)]
    for device in greeted:
        pl.semaphore_signal(barrier, inc=1, device_id=device, device_id_type=MESH)
    pacc[...] = jnp.zeros_like(pacc)
    racc[...] = jnp.zeros_like(racc)
    load.wait()
    pl.semaphore_wait(barrier, len(greeted))

    odd = lax.rem(lax.rem(p, depth), 2) == 1
    is_low = p < depth
    sends_last = odd == is_low
    receives_last = odd != is_low

    def far_copy(d, i):
        at = pl.ds(pl.multiple_of(i * piece, piece), piece)
        return remote(raw.at[l, at], far_raw.at[d, i, l], zs_sem.at[d, i], zr_sem.at[d, i],
                      (lax.rem(p + d + 1, rows), c, l))

    def relay(d, i):
        return remote(far_raw.at[d, i, l], far_raw.at[d, i, l], xs_sem.at[d, i], xr_sem.at[d, i], (p, c, other))

    for d in range(depth - 1):
        for i in range(pieces):
            far_copy(d, i).start()

    @pl.when(sends_last)
    def _():
        for i in range(pieces):
            far_copy(depth - 1, i).start()

    exchange = remote(raw.at[l], raw.at[l], ex_sem.at[0], ex_sem.at[1], (p, c, other))
    exchange.start()
    exchange.wait_recv()

    step = 32

    def scale(low, high):
        low, high = low.astype(jnp.float32), high.astype(jnp.float32)
        total = jnp.sum(low, axis=1, keepdims=True) + jnp.sum(high, axis=1, keepdims=True)
        squares = jnp.sum(low * low + high * high, axis=1, keepdims=True)
        average = total / samples
        variance = squares / samples - average * average
        gain = lax.rsqrt(variance + epsilon)
        return (((low - average) * gain).astype(jnp.bfloat16), ((high - average) * gain).astype(jnp.bfloat16))

    def standardize(h):
        for i in range(half // step):
            at = pl.ds(pl.multiple_of(h * half + i * step, step), step)
            low, high = scale(raw[0, at, :], raw[1, at, :])
            own[at, 0:part] = low
            own[at, part:samples] = high

    def standardize_far(d, i):
        for j in range(piece // step):
            at = pl.ds(j * step, step)
            low, high = scale(far_raw[d, i, 0, at, :], far_raw[d, i, 1, at, :])
            far[d, i, at, 0:part] = low
            far[d, i, at, part:samples] = high

    standardize(l)
    mine_at = pl.ds(pl.multiple_of(l * half, half), half)
    cut = half // 2

    def panel_copy(k, s):
        at = pl.ds(pl.multiple_of(l * half + s * cut, cut), cut)
        return remote(own.at[at], panel.at[pl.ds(order.index(k) * half + s * cut, cut)], ps_sem.at[k - 1, s], pr_sem.at[k - 1, s],
                      (p, flip(c, k), l))

    def pass_on(s):
        source, target = (2, 1) if s == 0 else (1, 2)
        return remote(panel.at[pl.ds(source * half + s * cut, cut)], panel.at[pl.ds(last * half + s * cut, cut)],
                      ps_sem.at[2, s], pr_sem.at[2, s], (p, flip(c, target), l))

    direct = [k for k in range(1, cols) if k != 3]
    panel_copies = {(k, s): panel_copy(k, s) for k in direct for s in range(2)}
    panel_copies.update({(3, s): pass_on(s) for s in range(2)})
    for k, s in [(1, 1), (2, 0), (1, 0), (2, 1)] + [(k, s) for k in direct[2:] for s in range(2)]:
        panel_copies[k, s].start()

    standardize(other)
    panel[rows_of(0, 1), :] = own[mine_at, :]

    def adjacency(at, block):
        product = lax.dot_general(
            panel[at, :], block, (((1,), (1,)), ((), ())), preferred_element_type=jnp.float32
        )
        shifted = product * (0.5 / samples) + 0.5
        square = shifted * shifted
        fourth = square * square
        eighth = fourth * fourth
        return eighth * fourth

    def own_pairs(first, stop):
        at = rows_of(first, stop)
        value = adjacency(at, own[...])
        lanes = value[:, 0:128]
        for j in range(1, genes // 128):
            lanes = lanes + value[:, j * 128:(j + 1) * 128]
        pacc[at, :] += lanes

    def far_pairs(first, stop, e):
        d, i = event(e)
        at = rows_of(first, stop)
        value = adjacency(at, far[d, i])
        pacc[at, :] += value
        racc[d, i] += jnp.sum(value.reshape(value.shape[0] // 8, 8, piece), axis=0)

    count = pieces * jnp.where(receives_last, depth, depth - 1)

    def event(e):
        return lax.div(e, pieces), lax.rem(e, pieces)

    own_pairs(0, 1)
    for s in range(2):
        panel_copies[2 - s, s].wait_recv()
        panel_copies[3, s].start()

    def take(e):
        d, i = event(e)
        far_copy(d, i).wait_recv()
        relay(d, i).start()

    def ready(e):
        d, i = event(e)
        relay(d, i).wait_recv()
        standardize_far(d, i)

    take(0)
    ready(0)
    take(1)
    take(2)
    ready(1)
    for s in range(2):
        panel_copies[1 + s, s].wait_recv()
    for k in direct[2:]:
        for s in range(2):
            panel_copies[k, s].wait_recv()
    own_pairs(1, last)
    longer = count > 3

    @pl.when(longer)
    def _():
        take(3)

    @pl.loop(0, count - 2)
    def _(e):
        @pl.when(e > 1)
        def _():
            @pl.when(e > 3)
            def _():
                take(e)

            ready(e)

        far_pairs(0, last, e)

    for s in range(2):
        panel_copies[3, s].wait_recv()
    own_pairs(last, cols)

    @pl.loop(0, count - 2)
    def _(e):
        far_pairs(last, cols, e)

    @pl.when(longer)
    def _():
        take(count - 2)
        take(count - 1)
        ready(count - 2)

    far_pairs(0, last, count - 2)
    far_pairs(last, cols, count - 2)
    ready(count - 1)
    far_pairs(0, last, count - 1)
    far_pairs(last, cols, count - 1)

    def fold(k):
        at = order.index(k)
        turned = pacc[rows_of(at, at + 1), :].T
        return jnp.sum(turned.reshape(128 // 8, 8, half), axis=0)

    def give_back(d):
        total = jnp.concatenate([racc[d, i] for i in range(pieces)], axis=1)
        home = lax.rem(p + rows - d - 1, rows)
        for h in range(2):
            rsrc[d, h] = total[:, h * half:(h + 1) * half]
            remote(rsrc.at[d, h], rdst.at[d, l], ts_sem.at[d, h], tr_sem.at[d, l], (home, c, h)).start()

    for d in range(depth - 1):
        give_back(d)

    @pl.when(receives_last)
    def _():
        give_back(depth - 1)

    part_copies = []
    for k in range(cols - 1, 0, -1):
        psrc[k - 1] = fold(k)
        copy = remote(psrc.at[k - 1], pdst.at[k - 1], qs_sem.at[k - 1], qr_sem.at[k - 1], (p, flip(c, k), l))
        copy.start()
        part_copies.append(copy)
    total = fold(0) - 1.0 / 8
    for copy in part_copies:
        copy.wait_recv()
    for k in range(1, cols):
        total = total + pdst[k - 1]

    def back_copy(d, h):
        return remote(rsrc.at[d, h], rdst.at[d, h], ts_sem.at[d, h], tr_sem.at[d, h], (p, c, other))

    for d in range(depth - 1):
        for h in range(2):
            back_copy(d, h).wait_recv()
            total = total + rdst[d, h]

    out_ref[...] = jnp.sum(total, axis=0)

    @pl.when(sends_last)
    def _():
        extra = jnp.zeros_like(total)
        for h in range(2):
            back_copy(depth - 1, h).wait_recv()
            extra = extra + rdst[depth - 1, h]
        out_ref[...] += jnp.sum(extra, axis=0)
        for i in range(pieces):
            far_copy(depth - 1, i).wait_send()

    exchange.wait_send()
    for copy in list(panel_copies.values()) + part_copies:
        copy.wait_send()
    for d in range(depth - 1):
        for i in range(pieces):
            far_copy(d, i).wait_send()
            relay(d, i).wait_send()
        for h in range(2):
            back_copy(d, h).wait_send()

    @pl.when(receives_last)
    def _():
        for i in range(pieces):
            relay(depth - 1, i).wait_send()
        for h in range(2):
            back_copy(depth - 1, h).wait_send()


def solution(mesh):
    rows, cols = mesh.shape["row"], mesh.shape["col"]
    depth = rows // 2
    piece = 128
    dma = lambda *shape: pltpu.SemaphoreType.DMA(shape)

    def on_device(expression):
        genes, part = expression.shape
        half, samples, pieces = genes // 2, 2 * part, genes // piece
        summed = pl.pallas_call(
            functools.partial(kernel, rows, cols),
            out_shape=jax.ShapeDtypeStruct((half,), jnp.float32),
            in_specs=[pl.BlockSpec(memory_space=pl.ANY)],
            out_specs=pl.BlockSpec(memory_space=pltpu.VMEM),
            scratch_shapes=[
                pltpu.VMEM((2, genes, part), jnp.bfloat16),
                pltpu.VMEM((genes, samples), jnp.bfloat16),
                pltpu.VMEM((cols * half, samples), jnp.bfloat16),
                pltpu.VMEM((depth, pieces, 2, piece, part), jnp.bfloat16),
                pltpu.VMEM((depth, pieces, piece, samples), jnp.bfloat16),
                pltpu.VMEM((cols * half, 128), jnp.float32),
                pltpu.VMEM((depth, pieces, 8, piece), jnp.float32),
                pltpu.VMEM((cols - 1, 8, half), jnp.float32),
                pltpu.VMEM((cols - 1, 8, half), jnp.float32),
                pltpu.VMEM((depth, 2, 8, half), jnp.float32),
                pltpu.VMEM((depth, 2, 8, half), jnp.float32),
                pltpu.SemaphoreType.DMA,
                dma(2),
                dma(cols - 1, 2), dma(cols - 1, 2),
                dma(depth, pieces), dma(depth, pieces),
                dma(depth, pieces), dma(depth, pieces),
                dma(cols - 1), dma(cols - 1),
                dma(depth, 2), dma(depth, 2),
            ],
            compiler_params=pltpu.CompilerParams(collective_id=0, has_side_effects=True),
        )(expression)
        return summed

    return jax.shard_map(
        on_device,
        mesh=mesh,
        in_specs=(P(("row", "col"), "layer"),),
        out_specs=P(("row", "col", "layer")),
        check_vma=False,
    )
```
